32 devices in a mesh: wide: 8 (over z, y), narrow: 4 (over x, core).
Axes of the slice: x: 2, y: 2, z: 4, core: 2. Of those that a mesh axis runs over, the one named last changes fastest.
Arguments:
- queries: bfloat16 [2048, 1024], P(('wide', 'narrow')), may hold values from -16 to 16
- documents: bfloat16 [2048, 1024], P(('wide', 'narrow')), may hold values from -16 to 16
- user_ids: int32 [2048], replicated, may hold values from 0 to 1663, as said below
Outputs:
- query_grad: bfloat16 [2048, 1024], P(('wide', 'narrow'))
- doc_grad: bfloat16 [2048, 1024], P(('wide', 'narrow'))
- loss: float32 [], replicated
The draws below stay inside these ranges and needn't reach their ends.
Inputs may be any that keep to these rules, and one draw needn't show every extreme that they name: `user_ids`: each user id names at most 4 rows; rows with a common id lie in the same quarter of the 2048 rows.
All inputs are finite; a program needn't handle non-finite values.
Results may differ from the reference program's by a relative error of at most 0.004.
The reference program's roundings to bfloat16 on the way (of `weights`) count: a program that leaves them out, or rounds other values in their place, can miss the bound.
Values may be sent and summed in bfloat16 or wider, within the bound.
A program may use at most 64 MiB of HBM per device.

```python
import math
import jax
import jax.numpy as jnp
from jax import lax

D = 1024
BATCH = 2048


def draw_pair(key):
    query_key = jax.random.fold_in(key, 11)
    doc_key = jax.random.fold_in(key, 12)
    query_raw = jnp.clip(jax.random.normal(query_key, (BATCH, D), jnp.float32), -4.0, 4.0)
    doc_raw = jnp.clip(jax.random.normal(doc_key, (BATCH, D), jnp.float32), -4.0, 4.0)
    return (query_raw, doc_raw)


def draw_queries(key, part):
    return draw_pair(key)[0].astype(jnp.bfloat16)


def draw_documents(key, part):
    return draw_pair(key)[1].astype(jnp.bfloat16)


def draw_user_ids(key, part):
    quarter = BATCH // 4
    pieces = []
    for band in range(4):
        order = jax.random.permutation(jax.random.fold_in(key, 21 + band), jnp.arange(quarter, dtype=jnp.int32))
        pieces.append(band * quarter + order // (band + 1))
    return jnp.concatenate(pieces).astype(jnp.int32)


def setup_inputs(seed: int = 0) -> dict:
    splits = jax.random.split(jax.random.key(seed), 4)
    return {
        "queries": draw_queries(jax.random.fold_in(splits[3], 71), 0),
        "documents": draw_documents(jax.random.fold_in(splits[3], 71), 0),
        "user_ids": draw_user_ids(jax.random.fold_in(splits[3], 71), 0),
    }


def reference(queries, documents, user_ids):
    score_scale = 3.0 / math.sqrt(D)
    block = math.gcd(BATCH, 512)
    blocks = BATCH // block
    query_blocks = queries.reshape(blocks, block, D)
    user_blocks = user_ids.reshape(blocks, block)

    def block_scores(query_rows):
        product = lax.dot_general(query_rows, documents, (((1,), (1,)), ((), ())), preferred_element_type=jnp.float32)
        return product * score_scale

    def statistics(inputs):
        query_rows, users = inputs
        scores = block_scores(query_rows)
        peak = lax.optimization_barrier(jnp.max(scores, axis=1))
        log_denom = peak + jnp.log(lax.optimization_barrier(jnp.sum(jnp.exp(scores - peak[:, None]), axis=1)))
        positive = users[:, None] == user_ids[None, :]
        counts = lax.optimization_barrier(jnp.sum(positive.astype(jnp.float32), axis=1))
        pos_sum = lax.optimization_barrier(jnp.sum(jnp.where(positive, scores, jnp.float32(0.0)), axis=1))
        return (log_denom, counts, pos_sum)
    log_denom, counts, pos_sum = lax.map(statistics, (query_blocks, user_blocks))
    total = jnp.sum(counts)
    loss = jnp.sum(counts * log_denom - pos_sum) / total

    def backward(doc_accum, inputs):
        query_rows, users, block_denom, block_counts = inputs
        scores = block_scores(query_rows)
        positive = (users[:, None] == user_ids[None, :]).astype(jnp.float32)
        probs = jnp.exp(scores - block_denom[:, None])
        weights = (jnp.float32(BATCH) * (block_counts[:, None] * probs - positive) / total).astype(jnp.bfloat16)
        query_part = jnp.dot(weights, documents, preferred_element_type=jnp.float32) * score_scale
        doc_part = lax.dot_general(weights, query_rows, (((0,), (0,)), ((), ())), preferred_element_type=jnp.float32) * score_scale
        return (doc_accum + doc_part, query_part.astype(jnp.bfloat16))
    doc_accum, query_parts = lax.scan(backward, jnp.zeros((BATCH, D), jnp.float32), (query_blocks, user_blocks, log_denom, counts))
    return (query_parts.reshape(BATCH, D), doc_accum.astype(jnp.bfloat16), loss)
```

```python
import functools
import math

import jax
import jax.numpy as jnp
from jax import lax
from jax.experimental import pallas as pl
from jax.experimental.pallas import tpu as pltpu
from jax.sharding import PartitionSpec as P

MESH = pl.DeviceIdType.MESH
COLUMN_CHUNKS = 4
ROW_PARTS = 2


def bit_count(size):
    bits = size.bit_length() - 1
    assert 1 << bits == size
    return bits


def tree(values, combine):
    while len(values) > 1:
        values = [combine(values[i], values[i + 1]) for i in range(0, len(values), 2)]
    return values[0]


def kernel(
    wide_count,
    narrow_count,
    query_bits,
    doc_bits,
    ids_hbm,
    queries_hbm,
    docs_hbm,
    query_out,
    doc_out,
    loss_out,
    ids_ref,
    qbuf,
    dbuf,
    stats,
    loss_query,
    loss_doc,
    wt_ref,
    w_ref,
    q_acc,
    d_acc,
    q_send,
    d_send,
    q_recv,
    d_recv,
    load_sem,
    send_sem,
    gq_recv,
    gd_recv,
    st_recv,
    lq_recv,
    ld_recv,
    rq_recv,
    rd_recv,
):
    rows, width = queries_hbm.shape
    qn, dn = 1 << len(query_bits), 1 << len(doc_bits)
    my_wide, my_narrow = lax.axis_index("wide"), lax.axis_index("narrow")
    core = lax.rem(my_narrow, 2)
    score_scale = 3.0 / math.sqrt(width)
    batch_rows = float(wide_count * narrow_count * rows)
    chunks = COLUMN_CHUNKS
    cols = width // chunks
    part_rows = rows // ROW_PARTS

    def other(bits, relative):
        place = {"wide": my_wide, "narrow": my_narrow}
        for k, (axis, bit) in enumerate(bits):
            if relative >> k & 1:
                index = place[axis]
                set_bit = lax.rem(index // (1 << bit), 2)
                place[axis] = index + (1 - 2 * set_bit) * (1 << bit)
        return place["wide"], place["narrow"]

    def remote(src, dst, recv, to):
        copy = pltpu.make_async_remote_copy(
            src_ref=src, dst_ref=dst, send_sem=send_sem, recv_sem=recv, device_id=to, device_id_type=MESH
        )
        copy.start()
        return copy

    loads = [
        pltpu.make_async_copy(docs_hbm, dbuf.at[0], load_sem.at[0]),
        pltpu.make_async_copy(queries_hbm, qbuf.at[0], load_sem.at[1]),
        pltpu.make_async_copy(ids_hbm, ids_ref, load_sem.at[2]),
    ]
    for load in loads:
        load.start()

    query_group = [other(query_bits, r) for r in range(qn)]
    doc_partner = [other(doc_bits, 1 << k) for k in range(len(doc_bits))]
    barrier = pltpu.get_barrier_semaphore()
    partners = query_group[1:] + doc_partner
    for partner in partners:
        pl.semaphore_signal(barrier, inc=1, device_id=partner, device_id_type=MESH)
    pl.semaphore_wait(barrier, len(partners))
    loads[0].wait()
    loads[1].wait()

    sent = []
    gathers = {}

    def pass_on(tower, r, part):
        buf, bits, recv = (
            (dbuf, doc_bits, gd_recv) if tower == "d" else (qbuf, query_bits, gq_recv)
        )
        span = pl.ds(part * part_rows, part_rows)
        for k in range(r.bit_length(), len(bits)):
            slot = r | 1 << k
            to = doc_partner[k] if tower == "d" else query_group[1 << k]
            copy = remote(
                buf.at[r, span], buf.at[slot, span], recv.at[slot, part], to
            )
            sent.append(copy)
            gathers[tower, slot, part] = copy

    for part in range(ROW_PARTS):
        pass_on("q", 0, part)
        pass_on("d", 0, part)

    loads[2].wait()
    pair = ids_ref.shape[1]
    id_rows = ids_ref.shape[0]
    quarter_rows = id_rows // 4

    def id_row(r):
        return ids_ref[pl.ds(r, 1), :].astype(jnp.float32)

    lane = lax.broadcasted_iota(jnp.int32, (pair, pair), 1)
    sublane = lax.broadcasted_iota(jnp.int32, (pair, pair), 0)
    diagonal = lane == sublane

    def as_column(row):
        return jnp.sum(jnp.where(diagonal, row, 0.0), axis=1, keepdims=True)

    def place_row(wide, narrow):
        return id_row((wide * narrow_count + narrow) // 2)

    low_half = lax.broadcasted_iota(jnp.int32, (1, pair), 1) < rows

    def swap_halves(row):
        return pltpu.roll(jnp.broadcast_to(row, (8, pair)), rows, 1)[0:1]

    first_core = core == 0
    query_pieces = []
    for r in range(0, qn, 2):
        a, b = place_row(*query_group[r]), place_row(*query_group[r + 1])
        left = jnp.where(first_core, a, swap_halves(a))
        right = jnp.where(first_core, swap_halves(b), b)
        query_pieces.append(jnp.where(low_half, left, right))
    query_ids = jnp.concatenate(query_pieces, axis=1)

    def count_step(r, carry):
        count_acc, total_acc = carry
        column = as_column(id_row(r))
        count_acc = count_acc + jnp.sum((column == query_ids).astype(jnp.float32), axis=0, keepdims=True)
        start = r // quarter_rows * quarter_rows

        def inner(k, acc):
            return acc + jnp.sum((column == id_row(start + k)).astype(jnp.float32), axis=0, keepdims=True)

        total_acc = lax.fori_loop(0, quarter_rows, inner, total_acc, unroll=quarter_rows <= 4)
        return count_acc, total_acc

    counts, total_row = lax.fori_loop(
        0,
        id_rows,
        count_step,
        (jnp.zeros((1, qn * rows), jnp.float32), jnp.zeros((1, pair), jnp.float32)),
    )
    total = jnp.sum(total_row, axis=1, keepdims=True)

    doc_columns = []
    for r in range(dn):
        wide, narrow = other(doc_bits, r)
        row = place_row(wide, narrow)
        half = lax.rem(narrow, 2)
        picked = jnp.where(half == 0, row, swap_halves(row))
        doc_columns.append(as_column(picked)[0:rows])
    doc_ids = jnp.concatenate(doc_columns, axis=0)

    arrivals = []
    for r in range(1, max(qn, dn)):
        for part in range(ROW_PARTS):
            if r < dn:
                arrivals.append(("d", r, part))
            if r < qn:
                arrivals.append(("q", r, part))
    for tower, r, part in arrivals:
        gathers[tower, r, part].wait_recv()
        pass_on(tower, r, part)

    all_queries = qbuf[...].reshape(qn * rows, width)
    all_docs = dbuf[...].reshape(dn * rows, width)
    scores = (
        lax.dot_general(
            all_docs, all_queries, (((1,), (1,)), ((), ())), preferred_element_type=jnp.float32
        )
        * score_scale
    )
    positive = doc_ids == query_ids
    peak = jnp.max(scores, axis=0, keepdims=True)
    exps = jnp.exp(scores - peak)
    denom = jnp.sum(exps, axis=0, keepdims=True)
    stats[0, 0:1] = peak
    stats[0, 1:2] = denom
    stat_copies = [
        remote(stats.at[0], stats.at[r], st_recv.at[r], query_group[r])
        for r in range(qn - 1, 0, -1)
    ]
    sent.extend(stat_copies)
    pos_sum = jnp.sum(jnp.where(positive, scores, 0.0), axis=0, keepdims=True)
    share = batch_rows / total
    pos_share = jnp.where(positive, share, 0.0)
    for copy in stat_copies:
        copy.wait_recv()

    def aligned_stats(r):
        pieces = []
        for t in range(qn // 2):
            piece = stats[r, :, pl.ds((t ^ r >> 1) * pair, pair)]
            pieces.append(pltpu.roll(piece, rows, 1) if r & 1 else piece)
        whole = jnp.concatenate(pieces, axis=1)
        return whole[0:1], whole[1:2]

    group_stats = [aligned_stats(r) for r in range(qn)]
    top = tree([p for p, _ in group_stats], jnp.maximum)
    row_denom = tree([d * jnp.exp(p - top) for p, d in group_stats], jnp.add)
    log_denom = top + jnp.log(row_denom)
    own = lax.broadcasted_iota(jnp.int32, (1, qn * rows), 1) < rows
    terms = jnp.where(own, counts * log_denom, 0.0) - pos_sum
    part_loss = jnp.sum(terms, axis=1, keepdims=True)
    loss_query[0] = jnp.broadcast_to(part_loss, loss_query.shape[1:])
    loss_copies = [
        remote(loss_query.at[0], loss_query.at[r], lq_recv.at[r], query_group[r])
        for r in range(qn - 1, 0, -1)
    ]
    sent.extend(loss_copies)

    factor = counts * jnp.exp(peak - log_denom) * share
    weights_t = exps * factor - pos_share
    wt_ref[...] = weights_t.astype(jnp.bfloat16)

    d_copies, q_copies = {}, {}

    def send_sum(tower, k, c):
        send, recv, rsem, copies = (
            (d_send, d_recv, rd_recv, d_copies)
            if tower == "d"
            else (q_send, q_recv, rq_recv, q_copies)
        )
        to = doc_partner[k] if tower == "d" else query_group[1 << k]
        span = pl.ds(1 << k, 1 << k)
        copy = remote(send.at[c, span], recv.at[c, span], rsem.at[k, c], to)
        sent.append(copy)
        copies[k, c] = copy

    def first_sum(tower, c, product):
        acc, send, bits = (d_acc, d_send, doc_bits) if tower == "d" else (q_acc, q_send, query_bits)
        half = 1 << (len(bits) - 1)
        blocks = (product * score_scale).reshape(2 * half, rows, cols)
        send[c, pl.ds(half, half)] = blocks[half:].astype(jnp.bfloat16)
        send_sum(tower, len(bits) - 1, c)
        acc[c] = blocks[:half]

    def doc_product(c):
        part_queries = qbuf[:, :, pl.ds(c * cols, cols)].reshape(qn * rows, cols)
        first_sum("d", c, jnp.dot(wt_ref[...], part_queries, preferred_element_type=jnp.float32))

    def query_product(c):
        part_docs = dbuf[:, :, pl.ds(c * cols, cols)].reshape(dn * rows, cols)
        first_sum("q", c, jnp.dot(w_ref[...], part_docs, preferred_element_type=jnp.float32))

    def next_sum(tower, k, c):
        acc, send, recv, copies = (
            (d_acc, d_send, d_recv, d_copies) if tower == "d" else (q_acc, q_send, q_recv, q_copies)
        )
        copies[k, c].wait_recv()
        if k == 0:
            out = doc_out if tower == "d" else query_out
            out[:, pl.ds(c * cols, cols)] = (acc[c, 0] + recv[c, 1].astype(jnp.float32)).astype(out.dtype)
            return
        half = 1 << (k - 1)
        upper = acc[c, pl.ds(half, half)] + recv[c, pl.ds((1 << k) + half, half)].astype(jnp.float32)
        send[c, pl.ds(half, half)] = upper.astype(jnp.bfloat16)
        send_sum(tower, k - 1, c)
        acc[c, pl.ds(0, half)] = acc[c, pl.ds(0, half)] + recv[c, pl.ds(1 << k, half)].astype(jnp.float32)

    loss_steps = list(range(len(doc_bits)))
    loss_state = {"sum": None, "copy": None, "step": 0}

    def loss_advance():
        step = loss_state["step"]
        if step == 0:
            for copy in loss_copies:
                copy.wait_recv()
            value = tree([loss_query[r] for r in range(qn)], jnp.add)
        elif step <= len(loss_steps):
            loss_state["copy"].wait_recv()
            value = loss_doc[step - 1, 0] + loss_doc[step - 1, 1]
        else:
            return
        loss_state["step"] = step + 1
        if step == len(loss_steps):
            loss_out[...] = value / total
            return
        loss_doc[step, 0] = value
        copy = remote(
            loss_doc.at[step, 0], loss_doc.at[step, 1], ld_recv.at[step], doc_partner[step]
        )
        sent.append(copy)
        loss_state["copy"] = copy

    d_levels, q_levels = len(doc_bits), len(query_bits)
    for c in range(chunks):
        doc_product(c)
        if c == 0:
            w_ref[...] = weights_t.T.astype(jnp.bfloat16)
        if c >= 1:
            next_sum("d", d_levels - 1, c - 1)
        query_product(c)
    next_sum("d", d_levels - 1, chunks - 1)
    loss_advance()
    for k in range(d_levels - 2, -1, -1):
        q_level = k - (d_levels - 1 - q_levels)
        for c in range(chunks):
            if q_level >= 0:
                next_sum("q", q_level, c)
            next_sum("d", k, c)
            if c % 2 == 1:
                loss_advance()
    while loss_state["step"] <= len(loss_steps):
        loss_advance()
    for copy in sent:
        copy.wait_send()


def store_results(query_ref, doc_ref, loss_ref, query_hbm, doc_hbm, loss_hbm, loss_one, sem):
    loss_one[...] = loss_ref[0:1, 0:1]
    copies = [
        pltpu.make_async_copy(query_ref, query_hbm, sem.at[0]),
        pltpu.make_async_copy(doc_ref, doc_hbm, sem.at[1]),
        pltpu.make_async_copy(loss_one, loss_hbm, sem.at[2]),
    ]
    for copy in copies:
        copy.start()
    for copy in copies:
        copy.wait()


def local(wide_count, narrow_count, queries, documents, user_ids):
    rows, width = queries.shape
    wide_bits, narrow_bits = bit_count(wide_count), bit_count(narrow_count)
    query_bits = [("wide", b) for b in range(wide_bits - 1, -1, -1) if b % 2 == 0]
    doc_bits = [("wide", b) for b in range(wide_bits) if b % 2 == 1]
    doc_bits += [("narrow", b) for b in range(narrow_bits - 1, -1, -1)]
    qb, db = len(query_bits), len(doc_bits)
    qn, dn = 1 << qb, 1 << db
    ids = user_ids.reshape(-1, 2 * rows)
    cols = width // COLUMN_CHUNKS
    dma = pltpu.SemaphoreType.DMA
    bf16, f32 = jnp.bfloat16, jnp.float32
    any_spec = pl.BlockSpec(memory_space=pl.ANY)
    vmem_spec = pl.BlockSpec(memory_space=pltpu.VMEM)
    query_grad, doc_grad, loss = pl.pallas_call(
        functools.partial(kernel, wide_count, narrow_count, query_bits, doc_bits),
        out_shape=(
            pltpu.VMEM((rows, width), bf16),
            pltpu.VMEM((rows, width), bf16),
            pltpu.VMEM((8, 128), f32),
        ),
        in_specs=[any_spec] * 3,
        out_specs=(vmem_spec,) * 3,
        scratch_shapes=[
            pltpu.VMEM(ids.shape, jnp.int32),
            pltpu.VMEM((qn, rows, width), bf16),
            pltpu.VMEM((dn, rows, width), bf16),
            pltpu.VMEM((qn, 8, qn * rows), f32),
            pltpu.VMEM((qn, 8, 128), f32),
            pltpu.VMEM((db, 2, 8, 128), f32),
            pltpu.VMEM((dn * rows, qn * rows), bf16),
            pltpu.VMEM((qn * rows, dn * rows), bf16),
            pltpu.VMEM((COLUMN_CHUNKS, qn // 2, rows, cols), f32),
            pltpu.VMEM((COLUMN_CHUNKS, dn // 2, rows, cols), f32),
            pltpu.VMEM((COLUMN_CHUNKS, qn, rows, cols), bf16),
            pltpu.VMEM((COLUMN_CHUNKS, dn, rows, cols), bf16),
            pltpu.VMEM((COLUMN_CHUNKS, qn, rows, cols), bf16),
            pltpu.VMEM((COLUMN_CHUNKS, dn, rows, cols), bf16),
            dma((3,)),
            dma(()),
            dma((qn, ROW_PARTS)),
            dma((dn, ROW_PARTS)),
            dma((qn,)),
            dma((qn,)),
            dma((db,)),
            dma((qb, COLUMN_CHUNKS)),
            dma((db, COLUMN_CHUNKS)),
        ],
        compiler_params=pltpu.CompilerParams(collective_id=0, has_side_effects=True, vmem_limit_bytes=60000 * 1024),
    )(ids, queries, documents)
    query_grad, doc_grad, loss = pl.pallas_call(
        store_results,
        out_shape=(
            jax.ShapeDtypeStruct((rows, width), bf16),
            jax.ShapeDtypeStruct((rows, width), bf16),
            jax.ShapeDtypeStruct((1, 1), f32),
        ),
        in_specs=[vmem_spec] * 3,
        out_specs=(any_spec,) * 3,
        scratch_shapes=[pltpu.VMEM((1, 1), f32), dma((3,))],
    )(*[pltpu.with_memory_space_constraint(x, pltpu.VMEM) for x in (query_grad, doc_grad, loss)])
    return query_grad, doc_grad, loss.reshape(())


def solution(mesh):
    return jax.shard_map(
        functools.partial(local, mesh.shape["wide"], mesh.shape["narrow"]),
        mesh=mesh,
        in_specs=(P(("wide", "narrow"), None), P(("wide", "narrow"), None), P()),
        out_specs=(P(("wide", "narrow"), None), P(("wide", "narrow"), None), P()),
        check_vma=False,
    )
```

```python
import functools
import math

import jax
import jax.numpy as jnp
from jax import lax
from jax.experimental import pallas as pl
from jax.experimental.pallas import tpu as pltpu
from jax.sharding import PartitionSpec as P

MESH = pl.DeviceIdType.MESH
COLUMN_CHUNKS = 4
ROW_PARTS = 4
DIRECT_CHUNKS = 1
DIRECT_PARTS = 1


def bit_count(size):
    bits = size.bit_length() - 1
    assert 1 << bits == size
    return bits


def tree(values, combine):
    while len(values) > 1:
        values = [combine(values[i], values[i + 1]) for i in range(0, len(values), 2)]
    return values[0]


def arrival_rank(r, part):
    top = r.bit_length() - 1
    if part >= ROW_PARTS - DIRECT_PARTS:
        return 3 * ROW_PARTS + part + r.bit_count()
    if r == 1 << top:
        return 2 * part + 1 if top == 0 else part + 1
    return arrival_rank(r ^ 1 << top, part) + 5


def kernel(
    wide_count,
    narrow_count,
    query_bits,
    doc_bits,
    ids_hbm,
    queries_hbm,
    docs_hbm,
    query_out,
    doc_out,
    loss_out,
    ids_ref,
    qbuf,
    dbuf,
    stats,
    loss_query,
    loss_doc,
    exp_send,
    exp_recv,
    wt_ref,
    w_ref,
    q_acc,
    d_acc,
    q_send,
    d_send,
    q_recv,
    d_recv,
    load_sem,
    send_sem,
    gq_recv,
    gd_recv,
    misc_recv,
    rq_recv,
    rd_recv,
):
    rows, width = queries_hbm.shape
    core_bit = ("narrow", 0)
    qn, dn = 1 << len(query_bits), 1 << len(doc_bits)
    my_wide, my_narrow = lax.axis_index("wide"), lax.axis_index("narrow")
    core = lax.rem(my_narrow, 2)
    score_scale = 3.0 / math.sqrt(width)
    batch_rows = float(wide_count * narrow_count * rows)
    chunks = COLUMN_CHUNKS
    cols = width // chunks
    part_rows = rows // ROW_PARTS

    def other(bits, relative):
        place = {"wide": my_wide, "narrow": my_narrow}
        for k, (axis, bit) in enumerate(bits):
            if relative >> k & 1:
                index = place[axis]
                set_bit = lax.rem(index // (1 << bit), 2)
                place[axis] = index + (1 - 2 * set_bit) * (1 << bit)
        return place["wide"], place["narrow"]

    sent = []

    def remote(src, dst, recv, to):
        copy = pltpu.make_async_remote_copy(
            src_ref=src, dst_ref=dst, send_sem=send_sem, recv_sem=recv, device_id=to, device_id_type=MESH
        )
        copy.start()
        sent.append(copy)
        return copy

    def wait_all(ref, sem):
        pltpu.make_async_copy(ref, ref, sem).wait()

    query_group = [other(query_bits + [core_bit], r) for r in range(2 * qn)]
    doc_group = [other(doc_bits, r) for r in range(dn)]
    sibling = query_group[qn]
    barrier = pltpu.get_barrier_semaphore()
    partners = query_group[1:] + doc_group[1:]
    for partner in partners:
        pl.semaphore_signal(barrier, inc=1, device_id=partner, device_id_type=MESH)
    loads = [
        pltpu.make_async_copy(docs_hbm, dbuf.at[0], load_sem.at[0]),
        pltpu.make_async_copy(queries_hbm, qbuf.at[0], load_sem.at[1]),
        pltpu.make_async_copy(ids_hbm, ids_ref, load_sem.at[2]),
    ]
    for load in loads:
        load.start()
    pl.semaphore_wait(barrier, len(partners))
    loads[0].wait()
    loads[1].wait()

    gathers = {}
    towers = {
        "q": (qbuf, len(query_bits), query_group, gq_recv, misc_recv.at[0]),
        "d": (dbuf, len(doc_bits), doc_group, gd_recv, misc_recv.at[1]),
    }

    def gather_copy(tower, r, slot, part):
        buf, bits, group, recv, _ = towers[tower]
        span = pl.ds(part * part_rows, part_rows)
        gathers[tower, slot, part] = remote(
            buf.at[r, span], buf.at[slot, span], recv.at[slot - 1, part], group[r ^ slot]
        )

    def to_sibling(tower, r, part):
        buf, bits, _, _, recv = towers[tower]
        span = pl.ds(part * part_rows, part_rows)
        remote(buf.at[r, span], buf.at[r + (1 << bits), span], recv, sibling)

    def pass_on(tower, r, part):
        bits = towers[tower][1]
        if part < ROW_PARTS - DIRECT_PARTS:
            for k in range(r.bit_length(), bits):
                gather_copy(tower, r, r | 1 << k, part)
        elif r == 0:
            for slot in sorted(range(1, 1 << bits), key=lambda s: (-s.bit_count(), s)):
                gather_copy(tower, 0, slot, part)

    for part in range(ROW_PARTS):
        pass_on("q", 0, part)
        pass_on("d", 0, part)
    for part in range(ROW_PARTS):
        to_sibling("q", 0, part)
        to_sibling("d", 0, part)

    loads[2].wait()
    pair = ids_ref.shape[1]
    id_rows = ids_ref.shape[0]
    quarter_rows = id_rows // 4

    def id_row(r):
        return ids_ref[pl.ds(r, 1), :].astype(jnp.float32)

    lane = lax.broadcasted_iota(jnp.int32, (pair, pair), 1)
    sublane = lax.broadcasted_iota(jnp.int32, (pair, pair), 0)
    diagonal = lane == sublane

    def as_column(row):
        return jnp.sum(jnp.where(diagonal, row, 0.0), axis=1, keepdims=True)

    def place_row(place):
        return id_row((place[0] * narrow_count + place[1]) // 2)

    first_core = core == 0
    low_half = lax.broadcasted_iota(jnp.int32, (1, pair), 1) < rows

    def swap_halves(row):
        return pltpu.roll(jnp.broadcast_to(row, (8, pair)), rows, 1)[0:1]

    def split_cores(a, b):
        a_swap, b_swap = swap_halves(a), swap_halves(b)
        mine = jnp.where(low_half, jnp.where(first_core, a, a_swap), jnp.where(first_core, b_swap, b))
        theirs = jnp.where(low_half, jnp.where(first_core, a_swap, a), jnp.where(first_core, b, b_swap))
        return mine, theirs

    def count_pair(r, acc):
        start = r // quarter_rows * quarter_rows
        row = id_row(r)

        def inner(k, acc):
            return acc + jnp.sum((as_column(id_row(start + k)) == row).astype(jnp.float32), axis=0, keepdims=True)

        return lax.fori_loop(0, quarter_rows, inner, acc, unroll=quarter_rows <= 4)

    zero_row = jnp.zeros((1, pair), jnp.float32)
    id_pieces, count_pieces = ([], []), ([], [])
    for r in range(0, qn, 2):
        a, b = query_group[r], query_group[r + 1]
        for piece, pieces in zip(split_cores(place_row(a), place_row(b)), id_pieces):
            pieces.append(piece)
        tally = [count_pair((p[0] * narrow_count + p[1]) // 2, zero_row) for p in (a, b)]
        for piece, pieces in zip(split_cores(*tally), count_pieces):
            pieces.append(piece)
    query_ids = jnp.concatenate(id_pieces[0] + id_pieces[1], axis=1)
    counts = jnp.concatenate(count_pieces[0] + count_pieces[1], axis=1)

    doc_pieces = ([], [])
    for r in range(dn):
        row = place_row(doc_group[r])
        column = as_column(jnp.where(first_core, row, swap_halves(row)))
        doc_pieces[0].append(column[0:rows])
        doc_pieces[1].append(column[rows:])
    doc_ids = jnp.concatenate(doc_pieces[0], axis=0)
    sibling_doc_ids = jnp.concatenate(doc_pieces[1], axis=0)

    def total_step(r, acc):
        column = as_column(id_row(r))
        start = r // quarter_rows * quarter_rows

        def inner(k, acc):
            return acc + jnp.sum((column == id_row(start + k)).astype(jnp.float32), axis=0, keepdims=True)

        return lax.fori_loop(0, quarter_rows, inner, acc, unroll=quarter_rows <= 4)

    total = jnp.sum(lax.fori_loop(0, id_rows, total_step, zero_row), axis=1, keepdims=True)

    arrivals = []
    for tower, n in (("q", qn), ("d", dn)):
        arrivals += [(arrival_rank(r, part), tower, r, part) for r in range(1, n) for part in range(ROW_PARTS)]
    for _, tower, r, part in sorted(arrivals):
        gathers[tower, r, part].wait_recv()
        pass_on(tower, r, part)
        to_sibling(tower, r, part)

    my_docs = dbuf[0:dn].reshape(dn * rows, width)

    def score_half(half):
        group_queries = qbuf[half * qn : (half + 1) * qn].reshape(qn * rows, width)
        return (
            lax.dot_general(
                my_docs, group_queries, (((1,), (1,)), ((), ())), preferred_element_type=jnp.float32
            )
            * score_scale
        )

    mine = score_half(0)
    wait_all(qbuf.at[pl.ds(qn, qn)], misc_recv.at[0])
    scores = jnp.concatenate([mine, score_half(1)], axis=1)
    peak = jnp.max(scores, axis=0, keepdims=True)
    exps = jnp.exp(scores - peak)
    denom = jnp.sum(exps, axis=0, keepdims=True)
    stat_rows = qn * rows * 2 // pair
    for t in range(stat_rows):
        stats[0, 0, t : t + 1] = peak[:, t * pair : (t + 1) * pair]
        stats[0, 1, t : t + 1] = denom[:, t * pair : (t + 1) * pair]
    for r in range(2 * qn - 1, 0, -1):
        remote(stats.at[0], stats.at[r], misc_recv.at[2], query_group[r])
    exp_send[...] = exps[:, qn * rows :]
    remote(exp_send, exp_recv, misc_recv.at[3], sibling)
    positive = doc_ids == query_ids
    pos_sum = jnp.sum(jnp.where(positive, scores, 0.0), axis=0, keepdims=True)
    share = batch_rows / total
    pos_share = jnp.where(positive, share, 0.0)
    sibling_pos_share = jnp.where(sibling_doc_ids == query_ids[:, : qn * rows], share, 0.0)
    wait_all(dbuf.at[pl.ds(dn, dn)], misc_recv.at[1])
    wait_all(exp_recv, misc_recv.at[3])
    wait_all(stats.at[pl.ds(1, 2 * qn - 1)], misc_recv.at[2])

    def aligned_stats(r):
        lines = []
        for s in range(2):
            pieces = []
            for t in range(stat_rows):
                piece = stats[r, s, pl.ds(t ^ r >> 1, 1)]
                pieces.append(swap_halves(piece) if r & 1 else piece)
            lines.append(jnp.concatenate(pieces, axis=1))
        return lines

    group_stats = [(peak, denom)] + [aligned_stats(r) for r in range(1, 2 * qn)]
    top = tree([p for p, _ in group_stats], jnp.maximum)
    row_denom = tree([d * jnp.exp(p - top) for p, d in group_stats], jnp.add)
    log_denom = top + jnp.log(row_denom)

    count_share = counts * share
    weights_t = exps * (count_share * jnp.exp(peak - log_denom)) - pos_share
    wt_ref[...] = weights_t.astype(jnp.bfloat16)

    levels = {"q": len(query_bits), "d": len(doc_bits)}
    parts = {
        "q": (q_acc, q_send, q_recv, rq_recv, query_group, query_out),
        "d": (d_acc, d_send, d_recv, rd_recv, doc_group, doc_out),
    }
    copies = {}

    def send_sum(tower, k, c):
        _, send, recv, sems, group, _ = parts[tower]
        span = pl.ds(1 << k, 1 << k)
        copies[tower, k, c] = remote(send.at[c, span], recv.at[c, span], sems.at[k, c], group[1 << k])

    def is_direct(c):
        return c >= chunks - DIRECT_CHUNKS

    def first_sum(tower, c, product):
        acc, send, recv, sems, group, _ = parts[tower]
        n = 1 << levels[tower]
        blocks = (product * score_scale).reshape(n, rows, cols)
        if is_direct(c):
            send[c, pl.ds(1, n - 1)] = blocks[1:].astype(jnp.bfloat16)
            for r in sorted(range(1, n), key=lambda s: (-s.bit_count(), s)):
                remote(send.at[c, r], recv.at[c, r], sems.at[0, c], group[r])
            acc[c, 0] = blocks[0]
        else:
            half = n // 2
            send[c, pl.ds(half, half)] = blocks[half:].astype(jnp.bfloat16)
            send_sum(tower, levels[tower] - 1, c)
            acc[c] = blocks[:half]

    def doc_product(c):
        part_queries = qbuf[:, :, pl.ds(c * cols, cols)].reshape(2 * qn * rows, cols)
        first_sum("d", c, jnp.dot(wt_ref[...], part_queries, preferred_element_type=jnp.float32))

    def query_product(c):
        part_docs = dbuf[:, :, pl.ds(c * cols, cols)].reshape(2 * dn * rows, cols)
        first_sum("q", c, jnp.dot(w_ref[...], part_docs, preferred_element_type=jnp.float32))

    def next_sum(tower, k, c):
        acc, send, recv, _, _, out = parts[tower]
        copies[tower, k, c].wait_recv()
        if k == 0:
            out[:, pl.ds(c * cols, cols)] = (acc[c, 0] + recv[c, 1].astype(jnp.float32)).astype(out.dtype)
            return
        half = 1 << (k - 1)
        upper = acc[c, pl.ds(half, half)] + recv[c, pl.ds((1 << k) + half, half)].astype(jnp.float32)
        send[c, pl.ds(half, half)] = upper.astype(jnp.bfloat16)
        send_sum(tower, k - 1, c)
        acc[c, pl.ds(0, half)] = acc[c, pl.ds(0, half)] + recv[c, pl.ds(1 << k, half)].astype(jnp.float32)

    def direct_sum(tower, c):
        acc, _, recv, sems, _, out = parts[tower]
        n = 1 << levels[tower]
        wait_all(recv.at[c, pl.ds(1, n - 1)], sems.at[0, c])
        value = acc[c, 0]
        for r in range(1, n):
            value = value + recv[c, r].astype(jnp.float32)
        out[:, pl.ds(c * cols, cols)] = value.astype(out.dtype)

    doc_product(0)
    half_lanes = qn * rows
    sibling_peak = group_stats[qn][0][:, :half_lanes]
    sibling_factor = count_share[:, :half_lanes] * jnp.exp(sibling_peak - log_denom[:, :half_lanes])
    sibling_weights = exp_recv[...] * sibling_factor - sibling_pos_share
    w_ref[:, : dn * rows] = weights_t[:, :half_lanes].T.astype(jnp.bfloat16)
    w_ref[:, dn * rows :] = sibling_weights.T.astype(jnp.bfloat16)
    query_product(0)

    own = lax.broadcasted_iota(jnp.int32, (1, 2 * qn * rows), 1) < rows
    terms = jnp.where(own, counts * log_denom, 0.0) - pos_sum
    part_loss = jnp.sum(terms, axis=1, keepdims=True)
    loss_query[0] = jnp.broadcast_to(part_loss, loss_query.shape[1:])
    for r in range(2 * qn - 1, 0, -1):
        remote(loss_query.at[0], loss_query.at[r], misc_recv.at[4], query_group[r])

    for c in range(1, chunks):
        doc_product(c)
        query_product(c)

    tree_chunks = [c for c in range(chunks) if not is_direct(c)]
    top_level = max(levels.values()) - 1
    for k in range(top_level, 0, -1):
        for c in tree_chunks:
            for tower in ("d", "q"):
                if k < levels[tower]:
                    next_sum(tower, k, c)
            if k == top_level and c == 0:
                wait_all(loss_query.at[pl.ds(1, 2 * qn - 1)], misc_recv.at[4])
                loss_doc[0] = tree([loss_query[r] for r in range(2 * qn)], jnp.add)
                for r in range(dn - 1, 0, -1):
                    remote(loss_doc.at[0], loss_doc.at[r], misc_recv.at[5], doc_group[r])
    for c in tree_chunks[:-1]:
        next_sum("q", 0, c)
        next_sum("d", 0, c)
    for c in range(chunks):
        if is_direct(c):
            direct_sum("q", c)
            direct_sum("d", c)
    wait_all(loss_doc.at[pl.ds(1, dn - 1)], misc_recv.at[5])
    loss_out[...] = tree([loss_doc[r] for r in range(dn)], jnp.add) / total
    for c in tree_chunks[-1:]:
        next_sum("q", 0, c)
        next_sum("d", 0, c)
    for copy in sent:
        copy.wait_send()


def store_results(query_ref, doc_ref, loss_ref, query_hbm, doc_hbm, loss_hbm, loss_one, sem):
    loss_one[...] = loss_ref[0:1, 0:1]
    copies = [
        pltpu.make_async_copy(query_ref, query_hbm, sem.at[0]),
        pltpu.make_async_copy(doc_ref, doc_hbm, sem.at[1]),
        pltpu.make_async_copy(loss_one, loss_hbm, sem.at[2]),
    ]
    for copy in copies:
        copy.start()
    for copy in copies:
        copy.wait()


def local(wide_count, narrow_count, queries, documents, user_ids):
    rows, width = queries.shape
    wide_bits, narrow_bits = bit_count(wide_count), bit_count(narrow_count)
    doc_bits = [("wide", b) for b in range(wide_bits - 1, -1, -1) if b % 2 == 0]
    query_bits = [("wide", b) for b in range(wide_bits) if b % 2 == 1]
    query_bits += [("narrow", b) for b in range(narrow_bits - 1, 0, -1)]
    qb, db = len(query_bits), len(doc_bits)
    qn, dn = 1 << qb, 1 << db
    ids = user_ids.reshape(-1, 2 * rows)
    cols = width // COLUMN_CHUNKS
    dma = pltpu.SemaphoreType.DMA
    bf16, f32 = jnp.bfloat16, jnp.float32
    any_spec = pl.BlockSpec(memory_space=pl.ANY)
    vmem_spec = pl.BlockSpec(memory_space=pltpu.VMEM)
    results = pl.pallas_call(
        functools.partial(kernel, wide_count, narrow_count, query_bits, doc_bits),
        out_shape=(
            pltpu.VMEM((rows, width), bf16),
            pltpu.VMEM((rows, width), bf16),
            pltpu.VMEM((8, 128), f32),
        ),
        in_specs=[any_spec] * 3,
        out_specs=(vmem_spec,) * 3,
        scratch_shapes=[
            pltpu.VMEM(ids.shape, jnp.int32),
            pltpu.VMEM((2 * qn, rows, width), bf16),
            pltpu.VMEM((2 * dn, rows, width), bf16),
            pltpu.VMEM((2 * qn, 2, qn, 2 * rows), f32),
            pltpu.VMEM((2 * qn, 8, 128), f32),
            pltpu.VMEM((dn, 8, 128), f32),
            pltpu.VMEM((dn * rows, qn * rows), f32),
            pltpu.VMEM((dn * rows, qn * rows), f32),
            pltpu.VMEM((dn * rows, 2 * qn * rows), bf16),
            pltpu.VMEM((qn * rows, 2 * dn * rows), bf16),
            pltpu.VMEM((COLUMN_CHUNKS, qn // 2, rows, cols), f32),
            pltpu.VMEM((COLUMN_CHUNKS, dn // 2, rows, cols), f32),
            pltpu.VMEM((COLUMN_CHUNKS, qn, rows, cols), bf16),
            pltpu.VMEM((COLUMN_CHUNKS, dn, rows, cols), bf16),
            pltpu.VMEM((COLUMN_CHUNKS, qn, rows, cols), bf16),
            pltpu.VMEM((COLUMN_CHUNKS, dn, rows, cols), bf16),
            dma((3,)),
            dma(()),
            dma((qn - 1, ROW_PARTS)),
            dma((dn - 1, ROW_PARTS)),
            dma((6,)),
            dma((qb, COLUMN_CHUNKS)),
            dma((db, COLUMN_CHUNKS)),
        ],
        compiler_params=pltpu.CompilerParams(collective_id=0, has_side_effects=True, vmem_limit_bytes=60000 * 1024),
    )(ids, queries, documents)
    query_grad, doc_grad, loss = pl.pallas_call(
        store_results,
        out_shape=(
            jax.ShapeDtypeStruct((rows, width), bf16),
            jax.ShapeDtypeStruct((rows, width), bf16),
            jax.ShapeDtypeStruct((1, 1), f32),
        ),
        in_specs=[vmem_spec] * 3,
        out_specs=(any_spec,) * 3,
        scratch_shapes=[pltpu.VMEM((1, 1), f32), dma((3,))],
    )(*[pltpu.with_memory_space_constraint(x, pltpu.VMEM) for x in results])
    return query_grad, doc_grad, loss.reshape(())


def solution(mesh):
    return jax.shard_map(
        functools.partial(local, mesh.shape["wide"], mesh.shape["narrow"]),
        mesh=mesh,
        in_specs=(P(("wide", "narrow"), None), P(("wide", "narrow"), None), P()),
        out_specs=(P(("wide", "narrow"), None), P(("wide", "narrow"), None), P()),
        check_vma=False,
    )
```
